32 devices in a mesh: seq: 8 (over z, x), tp: 4 (over y, core).
Axes of the slice: x: 2, y: 2, z: 4, core: 2. Of those that a mesh axis runs over, the one named last changes fastest.
Arguments:
- tokens: bfloat16 [1024, 4608], P('seq'), may hold values from -6 to 6
- counts: int32 [8], P('seq'), may hold values from 0 to 32, as said below
- selected: int32 [8, 32], P('seq'), may hold values from 0 to 127, as said below
- router_w: float32 [4608], replicated, may hold values from -0.09375 to 0.09375
- pre_gain: float32 [4608], replicated, may hold values from 0.25 to 1.75
- post_gain: float32 [4608], replicated, may hold values from 0.25 to 1.75
- gate_w: bfloat16 [4608, 36864], P(None, ('seq', 'tp')), may hold values from -0.09375 to 0.09375
- up_w: bfloat16 [4608, 36864], P(None, ('seq', 'tp')), may hold values from -0.09375 to 0.09375
- down_w: bfloat16 [36864, 4608], P(('seq', 'tp')), may hold values from -0.0625 to 0.0625
Outputs:
- layer_out: bfloat16 [1024, 4608], P('seq')
The draws below stay inside these ranges and needn't reach their ends.
Inputs may be any that keep to these rules, and one draw needn't show every extreme that they name: The counts sum to 128. For every shard s, the sum of the counts of the shards before s differs from s * 16 by at most 32. Each shard's first counts entries are distinct token positions of that shard in increasing order; the entries after them are padding and name no selected token.
All inputs are finite; a program needn't handle non-finite values.
Results may differ from the reference program's by a relative error of at most 0.003.
Values may be sent and summed in bfloat16 or wider, within the bound.
A program may use at most 128 MiB of HBM per device.

```python
import jax
import jax.numpy as jnp
from jax import lax

D = 4608
FF = 36864
TOK_DEV = 128
LOAD = 16
CAP = 32
SHARDS = 8
TOKENS = 1024


def draw_counts(key, part):
    shard_count = SHARDS
    slot_count = LOAD
    marked = jax.random.randint(jax.random.fold_in(key, 7), (), 3, shard_count - 2)
    moves = jax.random.randint(jax.random.fold_in(key, 11), (shard_count,), -slot_count, slot_count + 1)
    index = jnp.arange(shard_count)
    lower = jnp.full((shard_count,), -2 * slot_count, jnp.int32)
    upper = jnp.full((shard_count,), 2 * slot_count, jnp.int32)
    lower = jnp.where(index == marked - 3, -slot_count, lower)
    upper = jnp.where(index == marked - 3, slot_count, upper)
    lower = jnp.where(index == marked - 2, 0, lower)
    upper = jnp.where(index == marked - 2, slot_count, upper)
    lower = jnp.where(index == marked - 1, slot_count, lower)
    upper = jnp.where(index == marked - 1, slot_count, upper)
    moves = jnp.where(index == marked, slot_count, moves)
    lower = jnp.where(index == shard_count - 2, -slot_count, lower)
    upper = jnp.where(index == shard_count - 2, slot_count, upper)
    lower = jnp.where(index == shard_count - 1, 0, lower)
    upper = jnp.where(index == shard_count - 1, 0, upper)

    def advance(level, item):
        move_now, low_now, high_now = item
        following = jnp.clip(level + move_now, low_now, high_now)
        return (following, slot_count + following - level)
    final_level, drawn = lax.scan(advance, jnp.int32(0), (moves.astype(jnp.int32), lower, upper))
    return drawn.astype(jnp.int32)


def draw_selected(key, part):
    shard_keys = jax.random.split(jax.random.fold_in(key, 3), SHARDS)

    def one_shard(shard_key):
        order = jax.random.permutation(shard_key, TOK_DEV)
        return jnp.sort(order[:CAP])
    return jax.vmap(one_shard)(shard_keys).astype(jnp.int32)


def raised(values, key, source, target, blocks, factor):
    owner, partner = [(jnp.arange(values.shape[axis_at]) // (values.shape[axis_at] // blocks)).reshape([-1 if axis == axis_at else 1 for axis in range(values.ndim)]) for axis_at in (source, target)]
    chosen = jax.random.permutation(key, blocks)[partner]
    strong = (owner == chosen) | (owner == (partner + blocks // 2) % blocks)
    return jnp.where(strong, factor * values, values)


def steps_of(key, shape, pieces, least, largest):
    def one(dim, blocks):
        steps = jax.random.uniform(jax.random.fold_in(jax.random.fold_in(key, 6), dim), (blocks,), jnp.float32, least / len(pieces), largest / len(pieces))
        return jnp.repeat(jnp.exp(steps), shape[dim] // blocks).reshape((-1,) + (1,) * (len(shape) - dim - 1))

    factor_of = one(*pieces[0])
    for cut in pieces[1:]:
        factor_of = factor_of * one(*cut)
    return factor_of


def gaussian(own_key, extent, width, reach, shards=(), held_as=jnp.bfloat16):
    values = width * jax.random.normal(own_key, extent, jnp.float32)
    if shards:
        values = values * steps_of(own_key, extent, shards, -0.22, 0.18)
    return jnp.clip(values, -reach, reach).astype(held_as)


def noise_with(key, dims, width, limit, cuts, heavy, kind=jnp.bfloat16):
    values = width * jax.random.normal(key, dims, jnp.float32)
    if cuts:
        values = values * steps_of(key, dims, cuts, -0.22, 0.18)
    return jnp.clip(raised(values, jax.random.fold_in(key, 3), *heavy), -limit, limit).astype(kind)


def setup_inputs(seed: int = 0) -> dict:
    streams_of = jax.random.split(jax.random.key(seed), 10)
    tokens = gaussian(streams_of[0], (TOKENS, D), 1.0, 6.0, ((0, 8),))
    counts = draw_counts(jax.random.fold_in(streams_of[9], 71), 0)
    selected = draw_selected(jax.random.fold_in(streams_of[9], 71), 0)
    router_w = gaussian(streams_of[3], (D,), D ** -0.5, 0.09375, (), jnp.float32)
    pre_gain = jnp.clip(1.0 + 0.15 * jax.random.normal(streams_of[4], (D,), jnp.float32), 0.25, 1.75)
    post_gain = jnp.clip(1.0 + 0.15 * jax.random.normal(streams_of[5], (D,), jnp.float32), 0.25, 1.75)
    gate_w = gaussian(streams_of[6], (D, FF), D ** -0.5, 0.09375, ((1, 32),))
    up_w = gaussian(streams_of[7], (D, FF), D ** -0.5, 0.09375, ((1, 32),))
    down_w = noise_with(streams_of[8], (FF, D), FF ** -0.5, 0.0625, ((0, 32),), (0, 1, 32, 2.75))
    return dict(tokens=tokens, counts=counts, selected=selected, router_w=router_w, pre_gain=pre_gain, post_gain=post_gain, gate_w=gate_w, up_w=up_w, down_w=down_w)


EPS = 1e-06

def norm_rows(values, scale_vec):
    return values * lax.rsqrt(lax.optimization_barrier(jnp.mean(values * values, axis=-1, keepdims=True)) + EPS) * scale_vec

def reference(tokens, counts, selected, router_w, pre_gain, post_gain, gate_w, up_w, down_w):
    shard_count = counts.shape[0]
    tok_rows = tokens.shape[0] // shard_count
    total_rows = shard_count * LOAD
    ends = jnp.cumsum(counts).astype(jnp.int32)
    starts = (ends - counts).astype(jnp.int32)
    global_row = jnp.arange(total_rows, dtype=jnp.int32)
    owner = lax.optimization_barrier(jnp.sum((ends[None, :] <= global_row[:, None]).astype(jnp.int32), axis=1)).astype(jnp.int32)
    within = (global_row - starts[owner]).astype(jnp.int32)
    position = (selected[owner, within] + owner * tok_rows).astype(jnp.int32)
    work_rows = tokens[position].astype(jnp.float32)
    weight = jax.nn.sigmoid(jnp.dot(work_rows, router_w, precision=lax.Precision.HIGHEST))
    normed = norm_rows(work_rows, pre_gain).astype(jnp.bfloat16)
    gate_part = jnp.dot(normed, gate_w, preferred_element_type=jnp.float32)
    up_part = jnp.dot(normed, up_w, preferred_element_type=jnp.float32)
    hidden = (jax.nn.gelu(gate_part, approximate=True) * up_part).astype(jnp.bfloat16)
    mixed = jnp.dot(hidden, down_w, preferred_element_type=jnp.float32)
    update = weight[:, None] * norm_rows(mixed, post_gain)
    result = tokens.astype(jnp.float32).at[position].add(update)
    return result.astype(jnp.bfloat16)
```

```python
import functools

import jax
import jax.numpy as jnp
from jax import lax
from jax.experimental import pallas as pl
from jax.experimental.pallas import tpu as pltpu
from jax.sharding import PartitionSpec as P

EPS = 1e-06
MESH = pl.DeviceIdType.MESH
VMEM_BYTES = 67_043_328


def norm_rows(values, scale_vec):
    return values * lax.rsqrt(jnp.mean(values * values, axis=-1, keepdims=True) + EPS) * scale_vec


def pick_t(sel_ref, count, tok_rows):
    cap = sel_ref.shape[1]
    pos = lax.broadcasted_iota(jnp.int32, (tok_rows, cap), 0)
    slot = lax.broadcasted_iota(jnp.int32, (tok_rows, cap), 1)
    hit = (pos == sel_ref[...]) & (slot < count)
    return jnp.where(hit, 1.0, 0.0)


def vec_row(vecs, which, first, count):
    return jnp.concatenate([vecs[which, pl.ds(first + k, 1), :] for k in range(count)], axis=1)


def dot_t(a, b):
    return jnp.dot(a.T.astype(jnp.bfloat16), b, preferred_element_type=jnp.float32)


def main_kernel(
    dims, cnt_ref, sel_hbm, gain_hbm, router_hbm, post_hbm, tok_hbm, gate_hbm, up_hbm, down_hbm, out_ref,
    tok, gw, uw, dw, rows, sel_ref, vecs, cbuf, esrc, edst, xb, gacc, uacc, hid,
    sb, ra, own, ch, rb, plf, pz, rc, win, outb,
    tok_sem, v_sem, w_sem, send, recv,
):
    seq, tp, cap, load, quarter, pieces = dims
    nz = seq // 2
    reach = cap // load
    blocks = 2 * reach + 1
    width = blocks * load
    tok_rows = tok.shape[0]
    s = lax.axis_index("seq")
    t = lax.axis_index("tp")
    z, x = lax.div(s, 2), lax.rem(s, 2)
    y, c = lax.div(t, 2), lax.rem(t, 2)
    xpeer = z * 2 + (1 - x)
    ypeer = (1 - y) * 2 + c
    mate = y * 2 + (1 - c)
    far = (1 - y) * 2 + (1 - c)

    tok_copy = pltpu.make_async_copy(tok_hbm, tok, tok_sem)
    tok_copy.start()
    small = [pltpu.make_async_copy(sel_hbm, sel_ref, v_sem.at[0])]
    for i, src in enumerate((gain_hbm, router_hbm, post_hbm)):
        small.append(pltpu.make_async_copy(src, vecs.at[i], v_sem.at[i + 1]))
    for copy in small:
        copy.start()
    barrier = pltpu.get_barrier_semaphore()
    peers = [(lax.rem(s + d, seq), t) for d in range(1, seq)]
    peers += [(s, ypeer), (s, mate), (xpeer, ypeer)]
    for peer in peers:
        pl.semaphore_signal(barrier, inc=1, device_id=peer, device_id_type=MESH)
    gate_up, down = [], []
    for i, (src, dst) in enumerate(((gate_hbm, gw), (up_hbm, uw), (down_hbm, dw))):
        step = src.shape[0] // 4
        for j in range(4):
            part = pl.ds(j * step, step)
            copy = pltpu.make_async_copy(src.at[part], dst.at[part], w_sem.at[i * 4 + j])
            copy.start()
            (gate_up if i < 2 else down).append(copy)

    used = [0]

    def remote(src, dst, peer):
        k = used[0]
        used[0] += 1
        copy = pltpu.make_async_remote_copy(
            src_ref=src, dst_ref=dst, send_sem=send.at[k], recv_sem=recv.at[k],
            device_id=peer, device_id_type=MESH,
        )
        copy.start()
        return copy

    count = cnt_ref[0]
    cbuf[s] = jnp.full(cbuf.shape[1:], count, jnp.int32)
    pl.semaphore_wait(barrier, len(peers))
    counted = [remote(cbuf.at[s], cbuf.at[s], (lax.rem(s + d, seq), t)) for d in range(1, seq)]

    for copy in small:
        copy.wait()
    tok_copy.wait()
    compact = dot_t(pick_t(sel_ref, count, tok_rows), tok[...])
    rows[...] = compact
    inv = lax.rsqrt(jnp.mean(compact * compact, axis=-1, keepdims=True) + EPS)
    columns = pl.ds(pl.multiple_of(t * quarter, 128), quarter)
    lanes = quarter // 128
    gain = vec_row(vecs, 0, t * lanes, lanes)
    normed = (rows[:, columns] * inv * gain).astype(jnp.bfloat16)
    for copy in counted:
        copy.wait()
    start = jnp.zeros(cbuf.shape[1:], jnp.int32)
    for i in range(seq):
        start = start + cbuf[i] * (i < s).astype(jnp.int32)
    slot = lax.broadcasted_iota(jnp.int32, (cap, width), 0)
    at = lax.broadcasted_iota(jnp.int32, (cap, width), 1) + (s - reach) * load
    take = jnp.where((start[:1, :width] + slot == at) & (slot < count), 1.0, 0.0)

    esrc[...] = dot_t(take, normed).astype(jnp.bfloat16).reshape(blocks, load, quarter)
    near = []
    for d in range(-reach, reach + 1):
        if d:
            near.append(remote(esrc.at[reach + d], edst.at[len(near)], (lax.rem(s + d + seq, seq), t)))
    router = vec_row(vecs, 1, 0, compact.shape[1] // 128)
    weight = jax.nn.sigmoid(jnp.sum(compact * router, axis=-1, keepdims=True))
    block = esrc[reach].astype(jnp.float32)
    for i, copy in enumerate(near):
        copy.wait()
        block = block + edst[i].astype(jnp.float32)
    piece = quarter // pieces
    for p in range(pieces):
        xb[t, p, s] = block[:, p * piece:(p + 1) * piece].astype(jnp.bfloat16)

    rings = [
        [remote(xb.at[t, p, s], xb.at[t, p, s], (lax.rem(s + d, seq), t)) for d in range(1, seq)]
        for p in range(pieces)
    ]
    over_y, over_c, forward = [], [], []
    for p in range(pieces):
        for copy in rings[p]:
            copy.wait()
        over_y.append(remote(xb.at[t, p], xb.at[t, p], (s, ypeer)))
        over_c.append(remote(xb.at[t, p], xb.at[t, p], (s, mate)))
    for copy in gate_up:
        copy.wait()

    def add_piece(q, p, first=False):
        part = pl.ds(pl.multiple_of(q * quarter + p * piece, 128), piece)
        rows_in = xb[q, p].reshape(seq * load, piece)
        g = jnp.dot(rows_in, gw[part, :], preferred_element_type=jnp.float32)
        u = jnp.dot(rows_in, uw[part, :], preferred_element_type=jnp.float32)
        if first:
            gacc[...] = g
            uacc[...] = u
        else:
            gacc[...] += g
            uacc[...] += u

    for p in range(pieces):
        add_piece(t, p, p == 0)
        over_y[p].wait()
        forward.append(remote(xb.at[ypeer, p], xb.at[ypeer, p], (s, mate)))
    for p in range(pieces):
        over_c[p].wait()
        add_piece(mate, p)
        add_piece(ypeer, p)
    for p in range(pieces):
        forward[p].wait()
        add_piece(far, p)
    hid[...] = (jax.nn.gelu(gacc[...], approximate=True) * uacc[...]).astype(jnp.bfloat16)
    for copy in down:
        copy.wait()

    def product(q):
        part = pl.ds(pl.multiple_of(q * quarter, 128), quarter)
        m = jnp.dot(hid[...], dw[:, part], preferred_element_type=jnp.float32)
        return m.reshape(nz, 2, load, quarter)

    def to_mate(k):
        sb[k] = product(k * 2 + (1 - c)).astype(jnp.bfloat16)
        return remote(sb.at[k], ra.at[k], (s, mate))

    def chip_sum(k, copy):
        copy.wait()
        chip = own[k] + ra[k].astype(jnp.float32)
        own[k] = chip
        ch[k] = chip.astype(jnp.bfloat16)

    away = to_mate(1 - y)
    own[1 - y] = product((1 - y) * 2 + c)
    chip_sum(1 - y, away)
    plane = [
        remote(ch.at[1 - y, :, 1 - x], rb.at[2], (xpeer, ypeer)),
        remote(ch.at[1 - y, :, x], rb.at[1], (s, ypeer)),
    ]
    home = to_mate(y)
    own[y] = product(y * 2 + c)
    chip_sum(y, home)
    plane.append(remote(ch.at[y, :, 1 - x], rb.at[0], (xpeer, t)))
    for copy in plane:
        copy.wait()
    level = own[y, :, x] + rb[0].astype(jnp.float32) + rb[1].astype(jnp.float32) + rb[2].astype(jnp.float32)
    plf[...] = level
    pz[...] = level.astype(jnp.bfloat16)

    stack = []
    for d in range(1, nz):
        other = lax.rem(z + d, nz)
        stack.append(remote(pz.at[other], rc.at[d - 1], (other * 2 + x, t)))
    mixed = plf[z]
    for d in range(1, nz):
        stack[d - 1].wait()
        mixed = mixed + rc[d - 1].astype(jnp.float32)

    win[reach] = mixed.astype(jnp.bfloat16)
    near = []
    for d in range(-reach, reach + 1):
        if d:
            near.append(remote(win.at[reach], win.at[reach - d], (lax.rem(s + d + seq, seq), t)))
    for copy in near:
        copy.wait()
    outb[t] = jnp.dot(take.astype(jnp.bfloat16), win[...].reshape(width, quarter),
                      preferred_element_type=jnp.float32).astype(jnp.bfloat16)
    last_y = remote(outb.at[t], outb.at[t], (s, ypeer))
    last_c = remote(outb.at[t], outb.at[t], (s, mate))
    last_y.wait()
    last = remote(outb.at[ypeer], outb.at[ypeer], (s, mate))
    last_c.wait()
    last.wait()
    parts = [outb[q].astype(jnp.float32) for q in range(outb.shape[0])]
    square = sum(jnp.sum(part * part, axis=-1, keepdims=True) for part in parts)
    scale = lax.rsqrt(square / compact.shape[1] + EPS)
    for q, part in enumerate(parts):
        update = weight * (part * scale * vec_row(vecs, 2, q * lanes, lanes))
        high = update.astype(jnp.bfloat16)
        low = (update - high.astype(jnp.float32)).astype(jnp.bfloat16)
        pick = pick_t(sel_ref, count, tok_rows).astype(jnp.bfloat16)
        both = jnp.concatenate([pick, pick], axis=1)
        moved = jnp.dot(both, jnp.concatenate([high, low], axis=0), preferred_element_type=jnp.float32)
        cols = pl.ds(q * quarter, quarter)
        out_ref[:, cols] = (tok[:, cols].astype(jnp.float32) + moved).astype(jnp.bfloat16)


def final_kernel(cnt_ref, sel_ref, tok_ref, update_ref, out_ref):
    pick = pick_t(sel_ref, cnt_ref[0], tok_ref.shape[0]).astype(jnp.bfloat16)
    both = jnp.concatenate([pick, pick], axis=1)
    moved = jnp.dot(both, update_ref[...], preferred_element_type=jnp.float32)
    out_ref[...] = (tok_ref[...].astype(jnp.float32) + moved).astype(jnp.bfloat16)


def fused_body(tokens, counts, selected, router_w, pre_gain, post_gain, gate_w, up_w, down_w):
    seq, tp = lax.axis_size("seq"), lax.axis_size("tp")
    tok_rows, width = tokens.shape
    cap = selected.shape[1]
    load = cap // 2
    total = seq * load
    hidden = gate_w.shape[1]
    quarter = width // tp
    nz = seq // 2
    reach = cap // load
    bf16, f32 = jnp.bfloat16, jnp.float32
    pieces = 3 if quarter % 384 == 0 else 1
    copies = (seq - 1) * (1 + pieces) + 3 * pieces + 2 + 3 + (nz - 1) + 4 * reach + 3
    vmem = pl.BlockSpec(memory_space=pltpu.VMEM)
    smem = pl.BlockSpec(memory_space=pltpu.SMEM)
    anywhere = pl.BlockSpec(memory_space=pl.ANY)
    return pl.pallas_call(
        functools.partial(main_kernel, (seq, tp, cap, load, quarter, pieces)),
        out_shape=jax.ShapeDtypeStruct(tokens.shape, bf16),
        in_specs=[smem] + [anywhere] * 8,
        out_specs=vmem,
        scratch_shapes=[
            pltpu.VMEM((tok_rows, width), bf16),
            pltpu.VMEM((width, hidden), bf16),
            pltpu.VMEM((width, hidden), bf16),
            pltpu.VMEM((hidden, width), bf16),
            pltpu.VMEM((cap, width), f32),
            pltpu.VMEM(selected.shape, jnp.int32),
            pltpu.VMEM((3, width // 128, 128), f32),
            pltpu.VMEM((seq, 8, 128), jnp.int32),
            pltpu.VMEM((2 * reach + 1, load, quarter), bf16),
            pltpu.VMEM((2 * reach, load, quarter), bf16),
            pltpu.VMEM((tp, pieces, seq, load, quarter // pieces), bf16),
            pltpu.VMEM((total, hidden), f32),
            pltpu.VMEM((total, hidden), f32),
            pltpu.VMEM((total, hidden), bf16),
            pltpu.VMEM((2, nz, 2, load, quarter), bf16),
            pltpu.VMEM((2, nz, 2, load, quarter), bf16),
            pltpu.VMEM((2, nz, 2, load, quarter), f32),
            pltpu.VMEM((2, nz, 2, load, quarter), bf16),
            pltpu.VMEM((3, nz, load, quarter), bf16),
            pltpu.VMEM((nz, load, quarter), f32),
            pltpu.VMEM((nz, load, quarter), bf16),
            pltpu.VMEM((nz - 1, load, quarter), bf16),
            pltpu.VMEM((2 * reach + 1, load, quarter), bf16),
            pltpu.VMEM((tp, cap, quarter), bf16),
            pltpu.SemaphoreType.DMA,
            pltpu.SemaphoreType.DMA((4,)),
            pltpu.SemaphoreType.DMA((12,)),
            pltpu.SemaphoreType.DMA((copies,)),
            pltpu.SemaphoreType.DMA((copies,)),
        ],
        compiler_params=pltpu.CompilerParams(
            collective_id=0, has_side_effects=True, vmem_limit_bytes=VMEM_BYTES - (4 << 20)
        ),
    )(
        counts, selected, *(v.reshape(width // 128, 128) for v in (pre_gain, router_w, post_gain)),
        tokens, gate_w, up_w, down_w,
    )
def spread_body(tokens, counts, selected, router_w, pre_gain, post_gain, gate_w, up_w, down_w):
    tok_rows = tokens.shape[0]
    capacity = selected.shape[1]
    pair_count = lax.axis_size("tp")
    own_count = counts[0]
    chosen = selected[0]
    is_live = jnp.arange(capacity) < own_count
    positions = jnp.arange(tok_rows)
    picker = ((chosen[:, None] == positions[None, :]) & is_live[:, None]).astype(jnp.bfloat16)
    compact = jnp.dot(picker, tokens, preferred_element_type=jnp.float32).astype(jnp.bfloat16)
    piece_rows = compact.shape[0] // pair_count
    tp_index = lax.axis_index("tp")
    rows_float = compact.astype(jnp.float32)
    weight = jax.nn.sigmoid(jnp.dot(rows_float, router_w, precision=lax.Precision.HIGHEST))
    normed = norm_rows(rows_float, pre_gain).astype(jnp.bfloat16)
    segment = lax.all_gather(normed, "seq", axis=0, tiled=True)
    gate_part = jnp.dot(segment, gate_w, preferred_element_type=jnp.float32)
    up_part = jnp.dot(segment, up_w, preferred_element_type=jnp.float32)
    hidden = (jax.nn.gelu(gate_part, approximate=True) * up_part).astype(jnp.bfloat16)
    mixed = lax.psum_scatter(
        jnp.dot(hidden, down_w, preferred_element_type=jnp.float32),
        ("seq", "tp"),
        scatter_dimension=0,
        tiled=True,
    )
    own_weight = lax.dynamic_slice_in_dim(weight, tp_index * piece_rows, piece_rows, 0)
    finished = own_weight[:, None] * norm_rows(mixed, post_gain)
    updates = lax.all_gather(finished.astype(jnp.bfloat16), "tp", axis=0, tiled=True).astype(
        finished.dtype
    )
    scattered = jnp.einsum(
        "ct,cd->td", picker.astype(jnp.float32), updates, precision=lax.Precision.HIGHEST
    )
    return (tokens.astype(jnp.float32) + scattered).astype(jnp.bfloat16)


def body(*args):
    tokens, selected, gate_w = args[0], args[2], args[6]
    seq, tp = lax.axis_size("seq"), lax.axis_size("tp")
    load, hidden, width = selected.shape[1] // 2, gate_w.shape[1], tokens.shape[1]
    fits = (
        tp == 4 and seq % 2 == 0 and seq > 5 and load % 16 == 0 and 5 * load <= 128 and (seq * load) % 128 == 0
        and width % (tp * 128) == 0 and hidden % 128 == 0
        and 6 * width * hidden + 24 * seq * load * width < VMEM_BYTES
    )
    return fused_body(*args) if fits else spread_body(*args)


def solution(mesh):
    in_specs = (
        P("seq", None),
        P("seq"),
        P("seq", None),
        P(),
        P(),
        P(),
        P(None, ("seq", "tp")),
        P(None, ("seq", "tp")),
        P(("seq", "tp"), None),
    )
    out_specs = P("seq", None)
    return jax.shard_map(body, mesh=mesh, in_specs=in_specs, out_specs=out_specs, check_vma=False)
```
